512 devices in a mesh: groups: 2 (over y), seq: 32 (over z), head: 4 (over x), rep: 2 (over core).
Axes of the slice: x: 4, y: 2, z: 32, core: 2. Of those that a mesh axis runs over, the one named last changes fastest.
The devices are a block of a 4x8x32 slice.
Arguments:
- prefix_x: bfloat16 [8192, 8192], P(('groups', 'seq'), ('head', 'rep')), parts along dimension 0, may hold values from -6 to 6
- prefix_b: bfloat16 [8192, 8, 256], P(('groups', 'seq'), ('head', 'rep')), parts along dimension 0, may hold values from -0.09375 to 0.09375
- prefix_c: bfloat16 [8192, 8, 256], P(('groups', 'seq'), ('head', 'rep')), parts along dimension 0, may hold values from -0.375 to 0.375
- prefix_decay: float32 [8192, 128], P(('groups', 'seq'), ('head', 'rep')), parts along dimension 0, may hold values from 0 to 1.5, as said below
- bypass_weight: float32 [128], replicated, may hold values from 0.1 to 1.9
- prefix_key_rows: bfloat16 [8192, 4, 128], P(('groups', 'seq'), 'head'), parts along dimension 0, may hold values from -8 to 8
- prefix_values: bfloat16 [8192, 4, 128], P(('groups', 'seq'), 'head'), parts along dimension 0, may hold values from -6 to 6
- cand_x: bfloat16 [128, 32, 8192], P(('groups', 'seq', 'rep'), None, 'head'), parts along dimension 0, may hold values from -6 to 6
- cand_b: bfloat16 [128, 32, 8, 256], P(('groups', 'seq', 'rep'), None, 'head'), parts along dimension 0, may hold values from -0.09375 to 0.09375
- cand_c: bfloat16 [128, 32, 8, 256], P(('groups', 'seq', 'rep'), None, 'head'), parts along dimension 0, may hold values from -0.375 to 0.375
- cand_decay: float32 [128, 32, 128], P(('groups', 'seq', 'rep'), None, 'head'), parts along dimension 0, may hold values from 0 to 1.5, as said below
- cand_queries: bfloat16 [128, 32, 32, 128], P(('groups', 'seq', 'rep'), None, 'head'), parts along dimension 0, may hold values from -8 to 8
- cand_keys: bfloat16 [128, 32, 4, 128], P(('groups', 'seq', 'rep'), None, 'head'), parts along dimension 0, may hold values from -16 to 16
- cand_values: bfloat16 [128, 32, 4, 128], P(('groups', 'seq', 'rep'), None, 'head'), parts along dimension 0, may hold values from -6 to 6
- cand_length: int32 [128], P(('groups', 'seq', 'rep')), parts along dimension 0, may hold values from 16 to 32
Outputs:
- prefix_out: bfloat16 [8192, 8192], P(('groups', 'seq'), ('head', 'rep')), parts along dimension 0
- cand_ssm: bfloat16 [128, 32, 8192], P(('groups', 'seq', 'rep'), None, 'head'), parts along dimension 0
- cand_attn: bfloat16 [128, 32, 32, 128], P(('groups', 'seq', 'rep'), None, 'head'), parts along dimension 0
The draws below stay inside these ranges and needn't reach their ends.
There are 2 independent parts, one for each index of `groups`. The reference program is written for one: setup_inputs(seed, part) draws one part's arguments, and reference() takes and returns one part's arrays. A program takes and returns all parts, laid end to end along the dimension named above; an argument that names none is the same for every part. Nothing has to cross between parts.
Inputs may be any that keep to these rules, and one draw needn't show every extreme that they name: `prefix_decay`: positive. `cand_decay`: positive.
All inputs are finite; a program needn't handle non-finite values.
Results may differ from the reference program's by a relative error of at most 0.008.
Values may be sent and summed in bfloat16 or wider, within the bound.
A program may use at most 128 MiB of HBM per device.

```python
import jax
import jax.numpy as jnp
from jax import lax

GROUPS = 8
HEAD_DIM = 64
STATE = 256
KV_HEADS = 4
ATT_DIM = 128
TOK_DEV = 128
CT = 32
HEADS = 128
QHEADS = 32
PREFIX = 4096
CANDS = 64


def decay_law(key, steps, heads, chain, lead):
    keys = jax.random.split(key, 6)
    slow = jax.random.bernoulli(keys[0], 0.5, (heads,))
    approximate_guess = jnp.exp(jax.random.uniform(keys[1], lead + (steps, heads), minval=-0.69, maxval=0.69))
    slow_rate = jnp.exp(jax.random.uniform(keys[2], (heads,), minval=jnp.log(0.05), maxval=jnp.log(0.6))) / chain
    fast_rate = jnp.exp(jax.random.uniform(keys[3], (heads,), minval=jnp.log(1.0 / 50.0), maxval=jnp.log(1.0 / 30.0)))
    forgetting_speed = jnp.where(slow, slow_rate, fast_rate)
    proposal_locations = jax.random.randint(keys[4], (2, heads), 0, steps)
    symbol_quantities = jax.random.uniform(keys[5], (2, heads), minval=0.22, maxval=0.69)
    symbol_locations = jnp.arange(steps, dtype=jnp.int32)[:, None]
    driving_signals = (symbol_locations == proposal_locations[0][None, :]) * symbol_quantities[0][None, :] + (symbol_locations == proposal_locations[1][None, :]) * symbol_quantities[1][None, :]
    return (forgetting_speed * approximate_guess + driving_signals).astype(jnp.float32)


def draw_prefix_decay(key, part):
    return decay_law(jax.random.fold_in(key, 11), PREFIX, HEADS, PREFIX, ())


def draw_cand_decay(key, part):
    return decay_law(jax.random.fold_in(key, 13), CT, HEADS, PREFIX, (CANDS,))


def draw_prefix_key_rows(key, part):
    keys = jnp.clip(jax.random.normal(jax.random.fold_in(key, 31), (PREFIX, KV_HEADS, ATT_DIM)), -8.0, 8.0)
    return keys.astype(jnp.bfloat16)


def draw_cand_queries(key, part):
    queries = jnp.clip(jax.random.normal(jax.random.fold_in(key, 37), (CANDS, CT, QHEADS, ATT_DIM)), -8.0, 8.0)
    return queries.astype(jnp.bfloat16)


def touch_ends(values, own_key, least, top_value):
    longest = values.shape.index(max(values.shape))
    spots = []
    for shift in (0, 1):
        where = [jax.random.randint(jax.random.fold_in(own_key, axis), (), 0, length) for axis, length in enumerate(values.shape)]
        where[longest] = (where[longest] + shift) % values.shape[longest]
        spots.append(tuple(where))
    return values.at[spots[0]].set(least).at[spots[1]].set(top_value)


def steps_of(key, dims, shards, low, largest):
    level, own = 1.0, jax.random.fold_in(key, 6)
    for dim, parts in shards:
        draws = jnp.exp(jax.random.uniform(jax.random.fold_in(own, dim), (parts,), jnp.float32, low / len(shards), largest / len(shards)))
        level = level * jnp.repeat(draws, dims[dim] // parts).reshape([-1 if axis == dim else 1 for axis in range(len(dims))])
    return level


def centred(key, shape, scale, reach, shards=(), kind=jnp.bfloat16):
    values = scale * jax.random.normal(key, shape, jnp.float32)
    if shards:
        values = values * steps_of(key, shape, shards, -0.22, 0.18)
    return jnp.clip(values, -reach, reach).astype(kind)


def setup_inputs(seed: int = 0, part: int = 0) -> dict:
    streams_of = jax.random.split(jax.random.key(seed), 16)
    part_keys = jax.random.split(jax.random.fold_in(streams_of[15], part), 16)
    return {
        "prefix_x": centred(part_keys[0], (PREFIX, HEADS * HEAD_DIM), 1.0, 6.0, ((0, 32), (1, 8))),
        "prefix_b": centred(part_keys[1], (PREFIX, GROUPS, STATE), (4.0 / STATE), 0.09375, ((0, 32), (1, 8))),
        "prefix_c": centred(part_keys[2], (PREFIX, GROUPS, STATE), (1.0 / STATE ** 0.5), 0.375, ((0, 32), (1, 8))),
        "prefix_decay": draw_prefix_decay(jax.random.fold_in(jax.random.fold_in(streams_of[15], part), 71), part),
        "bypass_weight": jnp.clip(1.0 + 0.18 * jax.random.normal(streams_of[4], (HEADS,), jnp.float32), 0.1, 1.9),
        "prefix_key_rows": draw_prefix_key_rows(jax.random.fold_in(jax.random.fold_in(streams_of[15], part), 71), part),
        "prefix_values": centred(part_keys[6], (PREFIX, KV_HEADS, ATT_DIM), 1.0, 6.0, ((0, 32), (1, 4))),
        "cand_x": centred(part_keys[7], (CANDS, CT, HEADS * HEAD_DIM), 1.0, 6.0, ((0, 64), (2, 4))),
        "cand_b": centred(part_keys[8], (CANDS, CT, GROUPS, STATE), (4.0 / STATE), 0.09375, ((0, 64), (2, 4))),
        "cand_c": centred(part_keys[9], (CANDS, CT, GROUPS, STATE), (1.0 / STATE ** 0.5), 0.375, ((0, 64), (2, 4))),
        "cand_decay": draw_cand_decay(jax.random.fold_in(jax.random.fold_in(streams_of[15], part), 71), part),
        "cand_queries": draw_cand_queries(jax.random.fold_in(jax.random.fold_in(streams_of[15], part), 71), part),
        "cand_keys": centred(part_keys[12], (CANDS, CT, KV_HEADS, ATT_DIM), 2.5, 16.0, ((0, 64), (2, 4))),
        "cand_values": centred(part_keys[13], (CANDS, CT, KV_HEADS, ATT_DIM), 1.0, 6.0, ((0, 64), (2, 4))),
        "cand_length": touch_ends(jax.random.randint(part_keys[14], (CANDS,), CT // 2, CT + 1), jax.random.fold_in(part_keys[14], 1), CT // 2, CT).astype(jnp.int32),
    }


EPSILON = 1e-06
HIGH = lax.Precision.HIGHEST

def summarize(x, bmat, decay):
    length, groups, state = bmat.shape
    heads = decay.shape[1]
    per_group = heads // groups
    width = x.shape[1] // heads
    cum = jnp.cumsum(decay, axis=0)
    total = jnp.exp(-cum[-1])
    weights = jnp.exp(cum[-1][None, :] - cum)
    inputs = x.reshape(length, heads, width).astype(jnp.float32)
    weighted = (inputs * weights[:, :, None]).astype(jnp.bfloat16)
    weighted = lax.optimization_barrier(weighted).astype(jnp.float32)
    weighted = weighted.reshape(length, groups, per_group, width)
    local = jnp.einsum('sgn,sgkp->gknp', bmat.astype(jnp.float32), weighted, precision=HIGH)
    return (cum, total, local.reshape(heads, state, width))

def emit(x, bmat, cmat, cum, skip, start):
    length, groups, state = bmat.shape
    heads = cum.shape[1]
    per_group = heads // groups
    width = x.shape[1] // heads
    inputs = x.reshape(length, heads, width).astype(jnp.float32)
    gram = jnp.einsum('tgn,sgn->gts', cmat.astype(jnp.float32), bmat.astype(jnp.float32), precision=HIGH)
    gram = jnp.repeat(gram, per_group, axis=0)
    causal = jnp.arange(length)[:, None] >= jnp.arange(length)[None, :]
    gap = cum.T[:, :, None] - cum.T[:, None, :]
    state_mixing = jnp.where(causal, jnp.exp(-jnp.where(causal, gap, 0.0)), 0.0) * gram
    state_mixing = lax.optimization_barrier(state_mixing.astype(jnp.bfloat16)).astype(jnp.float32)
    intra = jnp.einsum('hts,shp->thp', state_mixing, inputs, precision=HIGH)
    start_set = start.astype(jnp.float32).reshape(groups, per_group, state, width)
    carried = jnp.einsum('tgn,gknp->tgkp', cmat.astype(jnp.float32), start_set, precision=HIGH)
    carried = carried.reshape(length, heads, width)
    result = intra + jnp.exp(-cum)[:, :, None] * carried + skip[None, :, None] * inputs
    return result.reshape(length, heads * width).astype(jnp.bfloat16)

def attend(query, keys, values, own_keys, own_values):
    steps, per_kv, dim = query.shape
    rows = query.reshape(steps * per_kv, dim)
    scale = dim ** (-0.5)
    far = jnp.dot(rows, keys.T, preferred_element_type=jnp.float32) * scale
    near = jnp.dot(rows, own_keys.T, preferred_element_type=jnp.float32) * scale
    position = jnp.arange(steps * per_kv) // per_kv
    near = jnp.where(position[:, None] >= jnp.arange(steps)[None, :], near, -jnp.inf)
    top = jnp.maximum(far.max(1), near.max(1))
    far_w = jnp.exp(far - top[:, None])
    near_w = jnp.exp(near - top[:, None])
    mass = far_w.sum(1) + near_w.sum(1)
    mixed = jnp.dot(far_w.astype(jnp.bfloat16), values, preferred_element_type=jnp.float32)
    mixed = mixed + jnp.dot(near_w.astype(jnp.bfloat16), own_values, preferred_element_type=jnp.float32)
    mixed = mixed / mass[:, None]
    mixed = mixed * lax.rsqrt(lax.optimization_barrier(jnp.mean(mixed * mixed, axis=-1, keepdims=True)) + EPSILON)
    return mixed.reshape(steps, per_kv, dim)

def reference(prefix_x, prefix_b, prefix_c, prefix_decay, bypass_weight, prefix_key_rows, prefix_values, cand_x, cand_b, cand_c, cand_decay, cand_queries, cand_keys, cand_values, cand_length):
    heads = prefix_decay.shape[1]
    groups = prefix_b.shape[1]
    state = prefix_b.shape[2]
    width = prefix_x.shape[1] // heads
    count = prefix_x.shape[0] // TOK_DEV
    pieces = (prefix_x.reshape(count, TOK_DEV, heads * width), prefix_b.reshape(count, TOK_DEV, groups, state), prefix_c.reshape(count, TOK_DEV, groups, state), prefix_decay.reshape(count, TOK_DEV, heads))

    def advance(start, piece):
        xb, bb, cb, db = piece
        cum, total, local = summarize(xb, bb, db)
        out = emit(xb, bb, cb, cum, bypass_weight, start)
        return (total[:, None, None] * start + local, out)
    final, outs = lax.scan(advance, jnp.zeros((heads, state, width), jnp.float32), pieces)
    prefix_out = outs.reshape(prefix_x.shape)
    steps = cand_x.shape[1]
    valid = jnp.arange(steps)[None, :] < cand_length[:, None]

    def candidate(piece):
        xb, bb, cb, db = piece
        cum = jnp.cumsum(db, axis=0)
        return emit(xb, bb, cb, cum, bypass_weight, final)
    cand_ssm = lax.map(candidate, (cand_x, cand_b, cand_c, cand_decay))
    cand_ssm = jnp.where(valid[:, :, None], cand_ssm, jnp.zeros((), jnp.bfloat16))
    kv_heads = prefix_key_rows.shape[1]
    dim = prefix_key_rows.shape[2]
    qheads = cand_queries.shape[2]
    per_kv = qheads // kv_heads
    keys_t = prefix_key_rows.transpose(1, 0, 2)
    values_t = prefix_values.transpose(1, 0, 2)

    def one_candidate(piece):
        query, own_keys, own_values = piece
        query = query.reshape(steps, kv_heads, per_kv, dim).transpose(1, 0, 2, 3)
        heads_out = lax.map(lambda args: attend(*args), (query, keys_t, values_t, own_keys.transpose(1, 0, 2), own_values.transpose(1, 0, 2)))
        return heads_out.transpose(1, 0, 2, 3).reshape(steps, qheads, dim)
    cand_attn = lax.map(one_candidate, (cand_queries, cand_keys, cand_values))
    cand_attn = jnp.where(valid[:, :, None, None], cand_attn, 0.0).astype(jnp.bfloat16)
    return (prefix_out, cand_ssm, cand_attn)
```

```python
import functools

import jax
import jax.numpy as jnp
from jax import lax
from jax.experimental import pallas as pl
from jax.experimental.pallas import tpu as pltpu
from jax.sharding import PartitionSpec as P

MESH = pl.DeviceIdType.MESH
EPSILON = 1e-06
HIGH = lax.Precision.HIGHEST
F32 = jnp.float32
BF16 = jnp.bfloat16

SEGMENTS = 4
ROWS = 16
WIDTH = 512
LATE = 2
BASE = 9
LAG = 4
HOP = 6


def iota(shape, dim):
    return lax.broadcasted_iota(jnp.int32, shape, dim)


def dot(a, b, contract=((1,), (0,)), precision=None):
    return lax.dot_general(a, b, (contract, ((), ())), precision=precision, preferred_element_type=F32)


def spread(heads, width, first, rows):
    shape = (rows, heads * width)
    return (iota(shape, 1) // width + first == iota(shape, 0)).astype(F32)


def whole(count):
    return [pl.BlockSpec(memory_space=pltpu.VMEM)] * count


def summarize(x_ref, b_ref, decay_ref, local, total, at):
    heads, length = decay_ref.shape
    width = x_ref.shape[1] // heads
    causal = (iota((length, length), 0) >= iota((length, length), 1)).astype(F32)
    cum = dot(causal, decay_ref[...], ((1,), (1,)), precision=HIGH)
    last = cum[length - 1 : length, :]
    columns = spread(heads, width, 0, heads)
    weights = dot(jnp.exp(last - cum), columns, precision=HIGH)
    product = dot(jnp.exp(-jnp.broadcast_to(last, (8, heads))), columns, precision=HIGH)
    weighted = (x_ref[...].astype(F32) * weights).astype(BF16)
    for half in range(x_ref.shape[1] // WIDTH):
        part = slice(half * WIDTH, (half + 1) * WIDTH)
        local[at + half] = dot(b_ref[...], weighted[:, part], ((0,), (0,)))
        total[at + half] = product[0:1, part]


def exchange_kernel(
    n,
    k_ref,
    v_ref,
    x_ref,
    b_ref,
    decay_ref,
    start_ref,
    decayed_ref,
    sums_ref,
    factors_ref,
    keys_ref,
    values_ref,
    local,
    total,
    gone,
    row,
    chain_recv,
    chain_send,
    row_sem,
    sum_recv,
    sum_send,
    factor_recv,
    factor_send,
    kv_up,
    kv_down,
    kv_send,
    mate_send,
    mate_recv,
):
    parts, state = start_ref.shape[:2]
    per_block = state // ROWS
    chunks = parts * per_block
    length = k_ref.shape[0]
    seg = n // SEGMENTS
    counts = ups, downs = n // 2, n - 1 - n // 2
    z = lax.axis_index("seq")
    core = lax.axis_index("rep")
    ways = (lax.rem(z + 1, n), lax.rem(z + n - 1, n))
    place, mine = lax.rem(z, seg), z // seg
    first, last = place == 0, place == seg - 1
    ours = core * parts

    def remote(src, dst, send, recv, **to):
        return pltpu.make_async_remote_copy(
            src_ref=src, dst_ref=dst, send_sem=send, recv_sem=recv, device_id=to, device_id_type=MESH
        )

    def await_all(ref, sem):
        pltpu.make_async_copy(ref, ref, sem).wait()

    def to_mate(ref, index):
        remote(ref, ref, mate_send.at[index], mate_recv.at[index], rep=1 - core).start()

    barrier = pltpu.get_barrier_semaphore()
    for to in ({"seq": ways[0]}, {"seq": ways[1]}, {"rep": 1 - core}):
        pl.semaphore_signal(barrier, inc=1, device_id=to, device_id_type=MESH)
    pl.semaphore_wait(barrier, 3)

    flows = ((kv_up, ups), (kv_down, downs))

    def rows_of(owner):
        return pl.ds(pl.multiple_of(owner * length, length), length)

    def each_kind(run):
        for kind, (own, gathered) in enumerate(((k_ref, keys_ref), (v_ref, values_ref))):

            @pl.when(core == kind)
            def _():
                run(kind, own, gathered)

    def own_block(kind, own, gathered):
        for way, (sems, count) in enumerate(flows):
            remote(own, gathered.at[rows_of(z)], kv_send.at[way], sems.at[0], seq=ways[way]).start()

    each_kind(own_block)
    summarize(x_ref, b_ref, decay_ref, local, total, 0)
    keys_ref[rows_of(z), :] = k_ref[...]
    values_ref[rows_of(z), :] = v_ref[...]

    def pass_block(way, i):
        sems, count = flows[way]
        owner = lax.rem(z + 1 + i, n) if way else lax.rem(z + n - 1 - i, n)

        def run(kind, own, gathered):
            ref = gathered.at[rows_of(owner)]
            await_all(ref, sems.at[i])

            @pl.when(i + 1 < count)
            def _():
                remote(ref, ref, kv_send.at[way], sems.at[i + 1], seq=ways[way]).start()

            to_mate(ref, kind)

        each_kind(run)

    def send_row(q, way):
        ref = factors_ref.at[q, pl.ds(ours, parts)]
        remote(ref, ref, factor_send.at[q, way], factor_recv.at[q], seq=ways[way]).start()

    def send_sum(q, way, ref, c):
        remote(ref, ref, sum_send.at[q, way], sum_recv.at[q, c], seq=ways[way]).start()

    def passed_on(q):
        up = lax.rem(z + n - (q * seg + seg - 1), n)
        is_down = up > ups
        far = jnp.where(is_down, n - up, up)
        sends = (
            jnp.logical_not(is_down) & (far < ups),
            ((far == 0) | is_down) & (far < downs),
        )
        return far == 0, far, sends

    def pass_on(q, send, *args):
        for way, good in enumerate(passed_on(q)[2]):

            @pl.when(good)
            def _():
                send(q, way, *args)

    def piece(c):
        return c // per_block, pl.ds(pl.multiple_of(lax.rem(c, per_block) * ROWS, ROWS), ROWS)

    def each_segment(run):
        for q in range(SEGMENTS):

            @pl.when(mine == q)
            def _():
                run(q)

    def chain_row():
        @pl.when(first)
        def _():
            decayed_ref[...] = jnp.ones_like(decayed_ref)

        @pl.when(jnp.logical_not(first))
        def _():
            await_all(decayed_ref, row_sem.at[1])

        product = decayed_ref[...] * total[...]

        @pl.when(jnp.logical_not(last))
        def _():
            row[...] = product
            remote(row, decayed_ref, row_sem.at[0], row_sem.at[1], seq=ways[0]).start()

        @pl.when(last)
        def _():
            factors_ref[mine, pl.ds(ours, parts)] = product
            each_segment(lambda q: pass_on(q, send_row))
            to_mate(factors_ref.at[mine, pl.ds(ours, parts)], 3)

    def chain_chunk(c):
        block, rows = piece(c)

        @pl.when(c == 0)
        def _():
            chain_row()

        def put(value):
            @pl.when(jnp.logical_not(last))
            def _():
                gone[block, rows] = value
                remote(
                    gone.at[block, rows],
                    start_ref.at[block, rows],
                    chain_send.at[0],
                    chain_recv.at[c],
                    seq=ways[0],
                ).start()

            @pl.when(last)
            def _():
                sums_ref[mine, ours + block, rows] = value
                ref = sums_ref.at[mine, ours + block, rows]
                each_segment(lambda q: pass_on(q, send_sum, ref, c))
                to_mate(ref, 2)

        @pl.when(first)
        def _():
            put(local[block, rows].astype(BF16))

        @pl.when(jnp.logical_not(first))
        def _():
            await_all(start_ref.at[block, rows], chain_recv.at[c])
            put((total[block] * start_ref[block, rows].astype(F32) + local[block, rows]).astype(BF16))

    def pass_row(q):
        ref = factors_ref.at[q, pl.ds(ours, parts)]
        await_all(ref, factor_recv.at[q])
        pass_on(q, send_row)
        to_mate(ref, 3)

    def pass_sum(q, c):
        block, rows = piece(c)

        @pl.when(c == 0)
        def _():
            pass_row(q)

        ref = sums_ref.at[q, ours + block, rows]
        await_all(ref, sum_recv.at[q, c])
        pass_on(q, send_sum, ref, c)
        to_mate(ref, 2)

    chain_at = BASE + LATE * seg * mine + LAG * place
    sum_at = []
    for q in range(SEGMENTS):
        at_home, far, _ = passed_on(q)
        begins = BASE + LATE * seg * q + LAG * (seg - 1 + far) + 1
        sum_at.append(jnp.where(at_home, LATE * n * n, begins))
    flow_at = []
    for way in (0, 1):
        begins = LATE * z + HOP + (LATE if way else -LATE)
        near = jnp.minimum(n - 1 - z if way else z, counts[way])
        flow_at.append((begins, begins - LATE * n if way else begins + LATE * n, near))

    def step(s, carry):
        c = s - chain_at

        @pl.when((c >= 0) & (c < chunks))
        def _():
            chain_chunk(c)

        for q in range(SEGMENTS):
            t = s - sum_at[q]

            @pl.when((t >= 0) & (t < chunks))
            def _():
                pass_sum(q, t)

        for way in (0, 1):
            pace = HOP + LATE if way else HOP - LATE
            before, after, near = flow_at[way]
            for begins, low, high in ((before, 0, near), (after, near, counts[way])):
                late = s - begins

                @pl.when((late >= low * pace) & (late < high * pace) & (lax.rem(late + n * n, pace) == 0))
                def _():
                    pass_block(way, late // pace)

        return carry

    steps = max(
        BASE + LATE * (n - seg) + LAG * (seg - 1 + ups) + chunks + 2, LATE * n + HOP * (ups + 1) + LATE * 2
    )
    lax.fori_loop(0, steps, step, 0)

    @pl.when(first)
    def _():
        start_ref[...] = jnp.zeros_like(start_ref)

    @pl.when(jnp.logical_not(last))
    def _():
        await_all(gone, chain_send.at[0])
        await_all(row, row_sem.at[0])

    def sent_sum(q, way):
        await_all(sums_ref.at[q, pl.ds(ours, parts)], sum_send.at[q, way])
        await_all(factors_ref.at[q, pl.ds(ours, parts)], factor_send.at[q, way])

    for q in range(SEGMENTS):
        pass_on(q, sent_sum)

    def sent_blocks(kind, own, gathered):
        for way, (sems, count) in enumerate(flows):
            await_all(gathered.at[pl.ds(0, count * length)], kv_send.at[way])
        await_all(gathered.at[pl.ds(0, (n - 1) * length)], mate_send.at[kind])

    each_kind(sent_blocks)

    @pl.when(core == 0)
    def _():
        await_all(values_ref.at[pl.ds(0, (n - 1) * length)], mate_recv.at[1])

    @pl.when(core == 1)
    def _():
        await_all(keys_ref.at[pl.ds(0, (n - 1) * length)], mate_recv.at[0])

    for sems in (mate_send, mate_recv):
        await_all(sums_ref.at[:, pl.ds(0, parts)], sems.at[2])
        await_all(factors_ref.at[:, pl.ds(0, parts)], sems.at[3])


def exchange(n, keys, values, x, b, decay):
    parts, state = x.shape[1] // WIDTH, b.shape[1]
    blocks = 2 * parts
    chunks = parts * state // ROWS
    length, dim = keys.shape
    dma = pltpu.SemaphoreType.DMA
    return pl.pallas_call(
        functools.partial(exchange_kernel, n),
        out_shape=(
            jax.ShapeDtypeStruct((parts, state, WIDTH), BF16),
            jax.ShapeDtypeStruct((parts, 1, WIDTH), F32),
            jax.ShapeDtypeStruct((SEGMENTS, blocks, state, WIDTH), BF16),
            jax.ShapeDtypeStruct((SEGMENTS, blocks, 1, WIDTH), F32),
            jax.ShapeDtypeStruct((n * length, dim), BF16),
            jax.ShapeDtypeStruct((n * length, dim), BF16),
        ),
        in_specs=whole(5),
        out_specs=tuple(whole(6)),
        scratch_shapes=[
            pltpu.VMEM((parts, state, WIDTH), F32),
            pltpu.VMEM((parts, 1, WIDTH), F32),
            pltpu.VMEM((parts, state, WIDTH), BF16),
            pltpu.VMEM((parts, 1, WIDTH), F32),
            dma((chunks,)),
            dma((1,)),
            dma((2,)),
            dma((SEGMENTS, chunks)),
            dma((SEGMENTS, 2)),
            dma((SEGMENTS,)),
            dma((SEGMENTS, 2)),
            dma((n // 2,)),
            dma((n - 1 - n // 2,)),
            dma((2,)),
            dma((4,)),
            dma((4,)),
        ],
        compiler_params=pltpu.CompilerParams(collective_id=0, has_side_effects=True),
        name="exchange",
    )(keys, values, x, b, decay)


def outputs_kernel(
    n,
    x_ref,
    b_ref,
    c_ref,
    decay_ref,
    skip_ref,
    start_ref,
    decayed_ref,
    sums_ref,
    factors_ref,
    cx_ref,
    cb_ref,
    cc_ref,
    cdecay_ref,
    q_ref,
    keys_ref,
    values_ref,
    ck_ref,
    cv_ref,
    length_ref,
    prefix_ref,
    cand_ref,
    attn_ref,
    carried_ref,
    final_ref,
    scores_ref,
):
    z = lax.axis_index("seq")
    core = lax.axis_index("rep")
    row_of_heads = lax.axis_index("head")
    parts = start_ref.shape[0]
    blocks = 2 * parts
    seg = n // SEGMENTS
    mine = z // seg

    for block in range(blocks):
        state = sums_ref[0, block].astype(F32)
        before = jnp.where(mine > 0, state, 0.0)
        for q in range(1, SEGMENTS):
            state = factors_ref[q, block] * state + sums_ref[q, block].astype(F32)
            if q + 1 < SEGMENTS:
                before = jnp.where(mine > q, state, before)
        final_ref[block] = state.astype(BF16)

        @pl.when(core == block // parts)
        def _():
            start = decayed_ref[block % parts] * before + start_ref[block % parts].astype(F32)
            carried_ref[:, (block % parts) * WIDTH : (block % parts + 1) * WIDTH] = dot(
                c_ref[...], start.astype(BF16)
            )

    heads, length = decay_ref.shape
    width = x_ref.shape[1] // heads
    lower = iota((length, length), 0) >= iota((length, length), 1)
    upper = iota((length, length), 0) <= iota((length, length), 1)
    decay = decay_ref[...]
    cum = dot(lower.astype(F32), decay, ((1,), (1,)), precision=HIGH)
    cum_t = dot(decay, upper.astype(F32), precision=HIGH)
    gram = dot(c_ref[...], b_ref[...], ((1,), (1,)))
    fade = dot(jnp.exp(-cum), spread(heads, width, 0, heads), precision=HIGH)
    skips = jnp.broadcast_to(skip_ref[...], (8, skip_ref.shape[1]))
    skip = dot(
        skips, spread(heads, width, (row_of_heads * 2 + core) * heads, skips.shape[1]), precision=HIGH
    )[0:1]
    for pair in range(heads // 2):
        pieces = []
        for h in (2 * pair, 2 * pair + 1):
            gap = jnp.where(lower, cum[:, h : h + 1] - cum_t[h : h + 1, :], 0.0)
            mixing = (jnp.where(lower, jnp.exp(-gap), 0.0) * gram).astype(BF16)
            pieces.append(dot(mixing, x_ref[:, h * width : (h + 1) * width]))
        part = slice(2 * pair * width, 2 * (pair + 1) * width)
        out = (
            jnp.concatenate(pieces, axis=1)
            + fade[:, part] * carried_ref[:, part]
            + skip[:, part] * x_ref[:, part].astype(F32)
        )
        prefix_ref[:, part] = out.astype(BF16)

    live = length_ref[0]
    steps, cheads = cdecay_ref.shape
    groups = cb_ref.shape[1] // b_ref.shape[1]
    per_group = cheads // groups
    states = b_ref.shape[1]
    span = 4
    ccausal = (iota((steps, steps), 0) >= iota((steps, steps), 1)).astype(F32)
    ccum = dot(ccausal, cdecay_ref[...], precision=HIGH)
    spread_steps = dot(ccum, spread(cheads, steps, 0, cheads), precision=HIGH)
    shape = spread_steps.shape
    own = lax.rem(iota(shape, 1), steps)
    flat = jnp.sum(jnp.where(own == iota(shape, 0), spread_steps, 0.0), axis=0, keepdims=True)
    visible = own <= iota(shape, 0)
    cgap = jnp.where(visible, spread_steps - flat, 0.0)
    kept = jnp.where(visible, jnp.exp(-cgap), 0.0)
    cfade = dot(jnp.exp(-ccum), spread(cheads, width, 0, cheads), precision=HIGH)
    cskip = dot(skips, spread(cheads, width, row_of_heads * cheads, skips.shape[1]), precision=HIGH)[0:1]
    alive = iota((steps, span * width), 0) < live
    diagonal = iota((span * steps, span * width), 0) // steps == iota((span * steps, span * width), 1) // width
    for group in range(groups):
        bg = cb_ref[:, group * states : (group + 1) * states]
        cg = cc_ref[:, group * states : (group + 1) * states]
        cgram = dot(cg, jnp.concatenate([bg] * span, axis=0), ((1,), (1,)))
        ccarried = [dot(cg, final_ref[group * parts + part]) for part in range(parts)]
        for k in range(per_group // span):
            h = group * per_group + k * span
            mixing = (kept[:, h * steps : (h + span) * steps] * cgram).astype(BF16)
            part = slice(h * width, (h + span) * width)
            xs = cx_ref[:, part]
            tall = jnp.where(diagonal, jnp.concatenate([xs] * span, axis=0), jnp.zeros((), BF16))
            offset = k * span * width
            inner = ccarried[offset // WIDTH][:, offset % WIDTH : offset % WIDTH + span * width]
            out = dot(mixing, tall) + cfade[:, part] * inner + cskip[:, part] * xs.astype(F32)
            cand_ref[:, part] = jnp.where(alive, out, 0.0).astype(BF16)

    rows, dim = q_ref.shape
    per_kv = rows // steps
    scale = dim ** (-0.5)
    query = q_ref[...]
    near = dot(query, ck_ref[...], ((1,), (1,))) * scale
    near = jnp.where(iota(near.shape, 0) // per_kv >= iota(near.shape, 1), near, -jnp.inf)
    top = jnp.max(near, axis=1, keepdims=True)
    tile = 512
    total = keys_ref.shape[0]
    tops = jnp.full((rows, 128), -jnp.inf, F32)
    for i in range(total // tile):
        scores = dot(query, keys_ref[i * tile : (i + 1) * tile, :], ((1,), (1,))) * scale
        scores_ref[:, i * tile : (i + 1) * tile] = scores
        for j in range(tile // 128):
            tops = jnp.maximum(tops, scores[:, j * 128 : (j + 1) * 128])
    top = jnp.maximum(top, jnp.max(tops, axis=1, keepdims=True))
    near = jnp.exp(near - top)
    mass = jnp.sum(near, axis=1, keepdims=True)
    mixed = dot(near.astype(BF16), cv_ref[...])
    sums = jnp.zeros((rows, 128), F32)
    for i in range(total // tile):
        weights = jnp.exp(scores_ref[:, i * tile : (i + 1) * tile] - top)
        for j in range(tile // 128):
            sums = sums + weights[:, j * 128 : (j + 1) * 128]
        mixed = mixed + dot(weights.astype(BF16), values_ref[i * tile : (i + 1) * tile, :])
    mass = mass + jnp.sum(sums, axis=1, keepdims=True)
    mixed = mixed / mass
    mixed = mixed * lax.rsqrt(jnp.mean(mixed * mixed, axis=1, keepdims=True) + EPSILON)
    attn_ref[...] = jnp.where(iota(mixed.shape, 0) < live * per_kv, mixed, 0.0).astype(BF16)


def outputs(n, args, length):
    x, cx, q, keys = args[0], args[9], args[13], args[14]
    start, sums = args[5], args[7]
    return pl.pallas_call(
        functools.partial(outputs_kernel, n),
        out_shape=(
            jax.ShapeDtypeStruct(x.shape, BF16),
            jax.ShapeDtypeStruct(cx.shape, BF16),
            jax.ShapeDtypeStruct(q.shape, BF16),
        ),
        in_specs=whole(len(args)) + [pl.BlockSpec(memory_space=pltpu.SMEM)],
        out_specs=tuple(whole(3)),
        scratch_shapes=[
            pltpu.VMEM(x.shape, F32),
            pltpu.VMEM(sums.shape[1:], BF16),
            pltpu.VMEM((q.shape[0], keys.shape[0]), F32),
        ],
        name="outputs",
    )(*args, length)


def on_device(
    n,
    prefix_x,
    prefix_b,
    prefix_c,
    prefix_decay,
    bypass_weight,
    prefix_key_rows,
    prefix_values,
    cand_x,
    cand_b,
    cand_c,
    cand_decay,
    cand_queries,
    cand_keys,
    cand_values,
    cand_length,
):
    b, c = prefix_b[:, 0], prefix_c[:, 0]
    steps = cand_x.shape[1]
    decay = prefix_decay.T
    start, decayed, sums, factors, keys, values = exchange(
        n, prefix_key_rows[:, 0], prefix_values[:, 0], prefix_x, b, decay
    )
    args = (
        prefix_x,
        b,
        c,
        decay,
        bypass_weight[None],
        start,
        decayed,
        sums,
        factors,
        cand_x[0],
        cand_b.reshape(steps, -1),
        cand_c.reshape(steps, -1),
        cand_decay[0],
        cand_queries.reshape(-1, cand_queries.shape[-1]),
        keys,
        values,
        cand_keys[0, :, 0],
        cand_values[0, :, 0],
    )
    prefix_out, cand_ssm, cand_attn = outputs(n, args, cand_length)
    return prefix_out, cand_ssm[None], cand_attn.reshape(cand_queries.shape)


def solution(mesh):
    rows = ("groups", "seq", "rep")
    placed = (
        P(("groups", "seq"), ("head", "rep")),
        P(("groups", "seq"), ("head", "rep"), None),
        P(("groups", "seq"), ("head", "rep"), None),
        P(("groups", "seq"), ("head", "rep")),
        P(),
        P(("groups", "seq"), "head", None),
        P(("groups", "seq"), "head", None),
        P(rows, None, "head"),
        P(rows, None, "head", None),
        P(rows, None, "head", None),
        P(rows, None, "head"),
        P(rows, None, "head", None),
        P(rows, None, "head", None),
        P(rows, None, "head", None),
        P(rows),
    )
    return jax.shard_map(
        functools.partial(on_device, mesh.shape["seq"]),
        mesh=mesh,
        in_specs=placed,
        out_specs=(
            P(("groups", "seq"), ("head", "rep")),
            P(rows, None, "head"),
            P(rows, None, "head", None),
        ),
        check_vma=False,
    )
```
